32 devices in a mesh: gx: 4 (over x, core), gy: 8 (over z, y).
Axes of the slice: x: 2, y: 2, z: 4, core: 2. Of those that a mesh axis runs over, the one named last changes fastest.
Arguments:
- residual: float32 [2, 524288], P(None, ('gx', 'gy')), may hold values from -15 to 15
- cam_jacobian: float32 [2, 9, 524288], P(None, None, ('gx', 'gy')), may hold values from -0.3 to 0.3
- point_jacobian: float32 [2, 3, 524288], P(None, None, ('gx', 'gy')), may hold values from -1.5 to 1.5
- obs_camera: int32 [524288], P(('gx', 'gy')), may hold values from 0 to 4095
- obs_slot: int32 [524288], P(('gx', 'gy')), may hold values from 0 to 127, as said below
- tile_offset: int32 [1024], P(('gx', 'gy')), may hold values from 0 to 1920, as said below
- damping: float32 [65536], P(('gx', 'gy')), may hold values from 0.3 to 3
- camera_slot: int32 [4096], replicated, may hold values from 0 to 4095, as said below
Outputs:
- reduced: float32 [9, 4096], P(None, ('gx', 'gy'))
- cost: float32 [], replicated
- grad_norm: float32 [], replicated
The draws below stay inside these ranges and needn't reach their ends.
Inputs may be any that keep to these rules, and one draw needn't show every extreme that they name: `obs_slot`: on each device observations are ordered by point; every observation's point lies in its tile's window of 128 points starting at tile_offset. `tile_offset`: windows lie within the device's 2048 points and do not fall from tile to tile. `camera_slot`: each position of the owners' layout is taken by exactly one camera.
All inputs are finite; a program needn't handle non-finite values.
Results may differ from the reference program's by a relative error of at most 0.000096.
Values sent between devices are 32-bit elements; how exact they have to be, the bound alone decides.
A program may use at most 64 MiB of HBM per device.

```python
import math
import jax
import jax.numpy as jnp
from jax import lax

OBS_DEV = 16384
TILE = 512
PW = 128
PTS_DEV = 2048
OBS = 524288
PTS = 65536
CAMS = 4096


def layout_draw(key):
    local_key = jax.random.fold_in(key, 11)
    position_all = jnp.arange(OBS, dtype=jnp.int32)
    local_pos = position_all % OBS_DEV
    jitter = jax.random.randint(local_key, (OBS,), 0, 3, dtype=jnp.int32)
    point_index = jnp.minimum(local_pos * PTS_DEV // OBS_DEV + jitter, PTS_DEV - 1)
    point_index = lax.cummax(point_index.reshape(OBS // OBS_DEV, OBS_DEV), axis=1)
    tiled = point_index.reshape(-1, TILE)
    offsets = jnp.clip(tiled[:, -1] - (PW - 1), 0, PTS_DEV - PW).astype(jnp.int32)
    slot_values = (tiled - offsets[:, None]).astype(jnp.int32)
    return (slot_values.reshape(-1), offsets)


def camera_draw(key):
    base_key = jax.random.fold_in(key, 37)
    keys = jax.random.split(base_key, 3)
    perm = jax.random.permutation(keys[0], CAMS).astype(jnp.int32)
    inverse = jnp.zeros((CAMS,), jnp.int32).at[perm].set(jnp.arange(CAMS, dtype=jnp.int32))
    first = jax.random.randint(keys[1], (OBS,), 0, CAMS, dtype=jnp.int32)
    second = jax.random.randint(keys[2], (OBS,), 0, CAMS, dtype=jnp.int32)
    chosen = jnp.maximum(first, second)
    return (inverse[chosen].astype(jnp.int32), perm)


def draw_obs_camera(key, part):
    return camera_draw(key)[0]


def draw_camera_slot(key, part):
    return camera_draw(key)[1]


def draw_obs_slot(key, part):
    return layout_draw(key)[0]


def draw_tile_offset(key, part):
    return layout_draw(key)[1]


def draw_residual(key, part):
    keys = jax.random.split(jax.random.fold_in(key, 23), 2)
    spread = jnp.exp(jax.random.uniform(keys[1], (OBS,), jnp.float32) * math.log(10.0))
    device_pos = (jnp.arange(OBS, dtype=jnp.int32) // OBS_DEV).astype(jnp.float32)
    device_scale = 1.0 + 2.0 * device_pos / max(OBS // OBS_DEV - 1, 1)
    base = jax.random.truncated_normal(keys[0], -4.0, 4.0, (2, OBS), jnp.float32)
    return (base * (spread * device_scale / 8.0)[None, :]).astype(jnp.float32)


def levels(own_key, shape, shards, least, high):
    loudness = 1.0
    for dim, parts in shards:
        draws = jax.random.uniform(jax.random.fold_in(jax.random.fold_in(own_key, 6), dim), (parts,), jnp.float32, least / len(shards), high / len(shards))
        loudness = loudness * jnp.repeat(jnp.exp(draws), shape[dim] // parts).reshape((-1,) + (1,) * (len(shape) - 1 - dim))
    return loudness


def noise(own_key, shape, scale, bound, cuts=(), kind=jnp.bfloat16):
    factor_of = levels(own_key, shape, cuts, -0.22, 0.18) if cuts else 1.0
    values = jax.random.normal(own_key, shape, jnp.float32) * scale * factor_of
    return jnp.minimum(jnp.maximum(values, -bound), bound).astype(kind)


def setup_inputs(seed: int = 0) -> dict:
    key_list = jax.random.split(jax.random.key(seed), 9)
    residual = draw_residual(jax.random.fold_in(key_list[8], 71), 0)
    cam_jacobian = noise(key_list[1], (2, 9, OBS), 0.05, 0.3, ((2, 32),), jnp.float32)
    point_jacobian = noise(key_list[2], (2, 3, OBS), 0.25, 1.5, ((2, 32),), jnp.float32)
    obs_camera = draw_obs_camera(jax.random.fold_in(key_list[8], 71), 0)
    obs_slot = draw_obs_slot(jax.random.fold_in(key_list[8], 71), 0)
    tile_offset = draw_tile_offset(jax.random.fold_in(key_list[8], 71), 0)
    damping = jnp.clip(jnp.exp(math.log(3.0) - 2.3025851 * jax.random.uniform(key_list[6], (PTS,), jnp.float32) ** levels(key_list[6], (PTS,), ((0, 32),), -0.2, 0.2)), 0.3, 3.0)
    camera_slot = draw_camera_slot(jax.random.fold_in(key_list[8], 71), 0)
    return {"residual": residual, "cam_jacobian": cam_jacobian, "point_jacobian": point_jacobian, "obs_camera": obs_camera, "obs_slot": obs_slot, "tile_offset": tile_offset, "damping": damping, "camera_slot": camera_slot}


def block_solve(entries, rhs):
    comp_aa = entries[0]
    comp_ab = entries[1]
    comp_ac = entries[2]
    comp_bb = entries[3]
    comp_bc = entries[4]
    comp_cc = entries[5]
    cof_aa = comp_bb * comp_cc - comp_bc * comp_bc
    cof_ab = comp_ac * comp_bc - comp_ab * comp_cc
    cof_ac = comp_ab * comp_bc - comp_ac * comp_bb
    cof_bb = comp_aa * comp_cc - comp_ac * comp_ac
    cof_bc = comp_ab * comp_ac - comp_aa * comp_bc
    cof_cc = comp_aa * comp_bb - comp_ab * comp_ab
    determ = comp_aa * cof_aa + comp_ab * cof_ab + comp_ac * cof_ac
    first = (cof_aa * rhs[0] + cof_ab * rhs[1] + cof_ac * rhs[2]) / determ
    second = (cof_ab * rhs[0] + cof_bb * rhs[1] + cof_bc * rhs[2]) / determ
    third = (cof_ac * rhs[0] + cof_bc * rhs[1] + cof_cc * rhs[2]) / determ
    return jnp.stack([first, second, third])

def point_features(residual, point_jacobian):
    grad_obs = lax.optimization_barrier(jnp.sum(point_jacobian * residual[:, None, :], axis=0))
    pairs = [(0, 0), (0, 1), (0, 2), (1, 1), (1, 2), (2, 2)]
    products = [lax.optimization_barrier(jnp.sum(point_jacobian[:, left] * point_jacobian[:, right], axis=0)) for left, right in pairs]
    return jnp.concatenate([grad_obs, jnp.stack(products)], axis=0)

def reference(residual, cam_jacobian, point_jacobian, obs_camera, obs_slot, tile_offset, damping, camera_slot):
    position_all = jnp.arange(OBS, dtype=jnp.int32)
    device_of = position_all // OBS_DEV
    point_of = (device_of * PTS_DEV + tile_offset[position_all // TILE] + obs_slot).astype(jnp.int32)
    features = point_features(residual, point_jacobian)
    point_sums = jax.ops.segment_sum(features.T, point_of, num_segments=PTS).T
    point_grad = point_sums[:3]
    diag_mask = jnp.array([1.0, 0.0, 0.0, 1.0, 0.0, 1.0], jnp.float32)[:, None]
    entries = point_sums[3:] + diag_mask * damping[None, :]
    step_point = block_solve(entries, point_grad)
    step_obs = jnp.take(step_point, point_of, axis=1)
    moved = lax.optimization_barrier(jnp.sum(point_jacobian * step_obs[None, :, :], axis=1))
    position = camera_slot[obs_camera].astype(jnp.int32)
    grad_obs = lax.optimization_barrier(jnp.sum(cam_jacobian * residual[:, None, :], axis=0))
    coupling_obs = lax.optimization_barrier(jnp.sum(cam_jacobian * moved[:, None, :], axis=0))
    camera_grad = jax.ops.segment_sum(grad_obs.T, position, num_segments=CAMS).T
    coupling = jax.ops.segment_sum(coupling_obs.T, position, num_segments=CAMS).T
    reduced = coupling - camera_grad
    cost = jnp.sum(residual * residual) / (2.0 * OBS)
    total = jnp.sum(camera_grad * camera_grad) + jnp.sum(point_grad * point_grad)
    grad_norm = jnp.sqrt(total / (9.0 * CAMS + 3.0 * PTS) + 1e-06)
    return (reduced, cost, grad_norm)
```

```python
import functools

import jax
import jax.numpy as jnp
from jax import lax
from jax.experimental import pallas as pl
from jax.experimental.pallas import tpu as pltpu
from jax.sharding import PartitionSpec as P

AXES = ("gx", "gy")
MESH = pl.DeviceIdType.MESH
F32 = jnp.float32
BF16 = jnp.bfloat16
LANES = 128
GROUP = 8
LOW_BITS = 8
LOW = 1 << LOW_BITS
PARAMS = 9
FEATURES = 16


def nt_dot(left, right):
    return lax.dot_general(left, right, (((1,), (1,)), ((), ())), preferred_element_type=F32)


def split_pieces(value, pieces):
    out = []
    rest = value
    for _ in range(pieces - 1):
        head = rest.astype(BF16)
        out.append(head)
        rest = rest - head.astype(F32)
    out.append(rest.astype(BF16))
    return out


def lane_take(row, index):
    table = jnp.broadcast_to(row, index.shape)
    return jnp.take_along_axis(table, index, axis=1)


def block_solve(entries, rhs):
    comp_aa, comp_ab, comp_ac, comp_bb, comp_bc, comp_cc = entries
    cof_aa = comp_bb * comp_cc - comp_bc * comp_bc
    cof_ab = comp_ac * comp_bc - comp_ab * comp_cc
    cof_ac = comp_ab * comp_bc - comp_ac * comp_bb
    cof_bb = comp_aa * comp_cc - comp_ac * comp_ac
    cof_bc = comp_ab * comp_ac - comp_aa * comp_bc
    cof_cc = comp_aa * comp_bb - comp_ab * comp_ab
    determ = comp_aa * cof_aa + comp_ab * cof_ab + comp_ac * cof_ac
    first = (cof_aa * rhs[0] + cof_ab * rhs[1] + cof_ac * rhs[2]) / determ
    second = (cof_ab * rhs[0] + cof_bb * rhs[1] + cof_bc * rhs[2]) / determ
    third = (cof_ac * rhs[0] + cof_bc * rhs[1] + cof_cc * rhs[2]) / determ
    return first, second, third


def point_kernel(
    toff_ref, res_ref, pj_ref, cam_ref, slot_ref, damp_ref, cslot_ref,
    w_ref, pos_ref, scal_ref, feat, sums, steps,
):
    rows = cam_ref.shape[0]
    tiles = toff_ref.shape[0]
    tile_rows = rows // tiles
    blocks = damp_ref.shape[0]
    table_rows = cslot_ref.shape[0]
    groups = rows // GROUP
    per_group = max(1, GROUP // tile_rows)

    sums[...] = jnp.zeros_like(sums)
    feat[...] = jnp.zeros_like(feat)

    def pair(ref, group, lead=()):
        return [
            ref[(*lead, pl.ds(group * (2 * GROUP) + part, GROUP, stride=2), slice(None))]
            for part in range(2)
        ]

    def group_step(group, cost):
        at = pl.ds(pl.multiple_of(group * GROUP, GROUP), GROUP)
        camera = cam_ref[at, :]
        high = camera >> 7
        low = camera & (LANES - 1)
        position = jnp.zeros_like(camera)
        for t in range(table_rows):
            position = jnp.where(high == t, lane_take(cslot_ref[t : t + 1, :], low), position)
        pos_ref[at, :] = position
        res = pair(res_ref, group)
        jac = [pair(pj_ref, group, (k,)) for k in range(3)]
        values = [jac[k][0] * res[0] + jac[k][1] * res[1] for k in range(3)]
        for k, l in ((0, 0), (0, 1), (0, 2), (1, 1), (1, 2), (2, 2)):
            values.append(jac[k][0] * jac[l][0] + jac[k][1] * jac[l][1])
        for f, value in enumerate(values):
            feat[pl.ds(group * (GROUP * FEATURES) + f, GROUP, stride=FEATURES), :] = value
        return cost + (res[0] * res[0] + res[1] * res[1])

    cost = lax.fori_loop(0, groups, group_step, jnp.zeros((GROUP, LANES), F32), unroll=2)

    points = lax.broadcasted_iota(jnp.int32, (LANES, LANES), 0)
    lane = lax.broadcasted_iota(jnp.int32, (FEATURES, LANES), 1)
    batch = 4 if tiles % 4 == 0 else 1

    def tile_batch(step, carry):
        totals = []
        for b in range(batch):
            tile = step * batch + b
            left, right = [], []
            for r in range(tile_rows):
                row = tile * tile_rows + r
                start = pl.multiple_of(row * FEATURES, FEATURES)
                pieces = split_pieces(feat[pl.ds(start, FEATURES), :], 3)
                left.append(jnp.concatenate(pieces, axis=0))
                slot = slot_ref[pl.ds(row, 1), :]
                right.append(jnp.where(points == slot, 1.0, 0.0).astype(BF16))
            out = nt_dot(jnp.concatenate(left, axis=1), jnp.concatenate(right, axis=1))
            totals.append(out[:FEATURES] + out[FEATURES : 2 * FEATURES] + out[2 * FEATURES :])
        for b in range(batch):
            offset = toff_ref[step * batch + b]
            block = offset >> 7
            shift = offset & (LANES - 1)
            rolled = pltpu.roll(totals[b], shift, 1)
            sums[block] += jnp.where(lane >= shift, rolled, 0.0)
            sums[block + 1] += jnp.where(lane < shift, rolled, 0.0)
        return carry

    lax.fori_loop(0, tiles // batch, tile_batch, 0)

    damp = damp_ref[...]
    columns = [sums[pl.ds(0, blocks), f, :] for f in range(9)]
    grad = columns[:3]
    entries = [
        col + damp if i in (0, 3, 5) else col for i, col in enumerate(columns[3:])
    ]
    step_point = block_solve(entries, grad)
    for k in range(3):
        steps[k, pl.ds(0, blocks), :] = step_point[k]
        steps[k, pl.ds(blocks, 1), :] = jnp.zeros((1, LANES), F32)
    square = grad[0] * grad[0] + grad[1] * grad[1] + grad[2] * grad[2]
    scal_ref[0:1, :] = jnp.sum(cost, axis=0, keepdims=True)
    scal_ref[1:2, :] = jnp.sum(square, axis=0, keepdims=True)

    sub = lax.broadcasted_iota(jnp.int32, (GROUP, LANES), 0)

    def take_step(group, carry):
        at = pl.ds(pl.multiple_of(group * GROUP, GROUP), GROUP)
        first = (group * GROUP) // tile_rows
        offsets = [toff_ref[first + t] for t in range(per_group)]
        shift = jnp.zeros((GROUP, LANES), jnp.int32) + (offsets[0] & (LANES - 1))
        for t in range(1, per_group):
            shift = jnp.where(sub >= t * tile_rows, offsets[t] & (LANES - 1), shift)
        index = slot_ref[at, :] + shift
        low = index & (LANES - 1)
        inside = index < LANES
        res = pair(res_ref, group)
        moved = [-res[0], -res[1]]
        for k in range(3):
            here = jnp.broadcast_to(steps[k, pl.ds(offsets[0] >> 7, 1), :], (GROUP, LANES))
            after = jnp.broadcast_to(steps[k, pl.ds((offsets[0] >> 7) + 1, 1), :], (GROUP, LANES))
            for t in range(1, per_group):
                later = sub >= t * tile_rows
                here = jnp.where(later, steps[k, pl.ds(offsets[t] >> 7, 1), :], here)
                after = jnp.where(later, steps[k, pl.ds((offsets[t] >> 7) + 1, 1), :], after)
            taken = jnp.where(
                inside,
                jnp.take_along_axis(here, low, axis=1),
                jnp.take_along_axis(after, low, axis=1),
            )
            jac = pair(pj_ref, group, (k,))
            moved = [moved[a] + jac[a] * taken for a in range(2)]
        w_ref[0, at, :] = moved[0]
        w_ref[1, at, :] = moved[1]
        return carry

    lax.fori_loop(0, groups, take_step, 0, unroll=2)


def camera_kernel(
    gx_size, gy_size, cost_scale, norm_scale,
    cj_ref, res_ref, w_ref, pos_ref, scal_ref,
    red_ref, cost_ref, norm_ref,
    acc, left, right, rowbuf, part, pair_in, chip_sum, recv, tot_send, tot_recv,
    pair_sems, chip_send, chip_recv, tot_ssem, tot_rsem,
):
    devices = gx_size * gy_size
    chips = devices // 2
    gx = lax.axis_index("gx")
    gy = lax.axis_index("gy")
    me = gx * gy_size + gy
    core = lax.rem(gx, 2)
    chip = (gx // 2) * gy_size + gy

    barrier = pltpu.get_barrier_semaphore()

    def greet(i, carry):
        peer = lax.rem(me + i, devices)
        pl.semaphore_signal(
            barrier, inc=1, device_id=(peer // gy_size, lax.rem(peer, gy_size)), device_id_type=MESH
        )
        return carry

    lax.fori_loop(1, devices, greet, 0)

    rows = pos_ref.shape[0]
    highs = devices * LANES // LOW
    lows = lax.broadcasted_iota(jnp.int32, (LOW, LANES), 0)
    tops = lax.broadcasted_iota(jnp.int32, (highs, LANES), 0)
    acc[...] = jnp.zeros_like(acc)

    def build(group, buf):
        at = pl.ds(pl.multiple_of(group * GROUP, GROUP), GROUP)
        even = pl.ds(group * (2 * GROUP), GROUP, stride=2)
        odd = pl.ds(group * (2 * GROUP) + 1, GROUP, stride=2)
        res0, res1 = res_ref[even, :], res_ref[odd, :]
        w0, w1 = w_ref[0, at, :], w_ref[1, at, :]
        for m in range(PARAMS):
            jac0, jac1 = cj_ref[m, even, :], cj_ref[m, odd, :]
            for j, value in ((m, jac0 * res0 + jac1 * res1), (m + PARAMS, jac0 * w0 + jac1 * w1)):
                head = value.astype(BF16).astype(F32)
                rowbuf[buf, j] = head
                rowbuf[buf, 2 * PARAMS + j] = value - head
        for r in range(GROUP):
            position = pos_ref[pl.ds(group * GROUP + r, 1), :]
            cols = slice(r * LANES, (r + 1) * LANES)
            right[buf, :, cols] = jnp.where(lows == (position & (LOW - 1)), 1.0, 0.0).astype(BF16)
            top = jnp.where(tops == (position >> LOW_BITS), 1.0, 0.0).astype(BF16)
            for j in range(4 * PARAMS):
                row = jnp.broadcast_to(rowbuf[buf, j, r : r + 1, :], (highs, LANES)).astype(BF16)
                left[buf, j * highs : (j + 1) * highs, cols] = row * top

    def two_groups(step, carry):
        for buf in range(2):
            build(step * 2 + buf, buf)
            acc[...] += nt_dot(left[buf], right[buf])
        return carry

    lax.fori_loop(0, rows // (2 * GROUP), two_groups, 0)

    for dest in range(devices):
        dgx, dgy = dest // gy_size, dest % gy_size
        half = slice((dest % 2) * LANES, (dest % 2 + 1) * LANES)
        top = dest // 2
        head = [acc[j * highs + top : j * highs + top + 1, half] for j in range(4 * PARAMS)]
        total = [head[j] + head[2 * PARAMS + j] for j in range(2 * PARAMS)]
        part[dgx % 2, (dgx // 2) * gy_size + dgy] = jnp.concatenate(total, axis=0)

    pl.semaphore_wait(barrier, devices - 1)

    swap = pltpu.make_async_remote_copy(
        src_ref=part.at[1 - core],
        dst_ref=pair_in,
        send_sem=pair_sems.at[0],
        recv_sem=pair_sems.at[1],
        device_id=(gx + 1 - 2 * core, gy),
        device_id_type=MESH,
    )
    swap.start()
    swap.wait()
    chip_sum[...] = part[core] + pair_in[...]

    def chip_copy(i):
        peer = lax.rem(chip + i, chips)
        return pltpu.make_async_remote_copy(
            src_ref=chip_sum.at[peer],
            dst_ref=recv.at[i],
            send_sem=chip_send.at[i],
            recv_sem=chip_recv.at[i],
            device_id=((peer // gy_size) * 2 + core, lax.rem(peer, gy_size)),
            device_id_type=MESH,
        )

    def chip_start(i, carry):
        chip_copy(i).start()
        return carry

    def chip_wait(i, total):
        chip_copy(i).wait()
        return total + recv[i]

    lax.fori_loop(1, chips, chip_start, 0)
    total = lax.fori_loop(1, chips, chip_wait, chip_sum[chip])
    red_ref[...] = total[PARAMS:]
    grad = total[:PARAMS]
    tot_send[0:1, :] = scal_ref[0:1, :]
    tot_send[1:2, :] = scal_ref[1:2, :] + jnp.sum(grad * grad, axis=0, keepdims=True)
    tot_recv[me] = tot_send[...]

    def tot_copy(i):
        peer = lax.rem(me + i, devices)
        return pltpu.make_async_remote_copy(
            src_ref=tot_send,
            dst_ref=tot_recv.at[me],
            send_sem=tot_ssem.at[i],
            recv_sem=tot_rsem.at[i],
            device_id=(peer // gy_size, lax.rem(peer, gy_size)),
            device_id_type=MESH,
        )

    def tot_start(i, carry):
        tot_copy(i).start()
        return carry

    def tot_wait(i, carry):
        tot_copy(i).wait()
        return carry

    lax.fori_loop(1, devices, tot_start, 0)
    lax.fori_loop(1, devices, tot_wait, 0)
    sums = tot_recv[0]
    for d in range(1, devices):
        sums = sums + tot_recv[d]
    sums = jnp.sum(sums, axis=1, keepdims=True)
    cost_ref[...] = sums[0:1] * cost_scale
    norm_ref[...] = jnp.sqrt(sums[1:2] * norm_scale + 1e-06)


def interleaved(array):
    lead = array.shape[:-2]
    n_obs = array.shape[-1]
    blocks = array.reshape(*lead, 2, n_obs // LANES, LANES)
    return jnp.swapaxes(blocks, -3, -2).reshape(*lead, 2 * n_obs // LANES, LANES)


def on_device(
    gx_size, gy_size,
    residual, cam_jacobian, point_jacobian, obs_camera, obs_slot, tile_offset, damping, camera_slot
):
    devices = gx_size * gy_size
    n_obs = residual.shape[1]
    rows = n_obs // LANES
    blocks = damping.shape[0] // LANES
    camera_count = camera_slot.shape[0]
    assert camera_count == devices * LANES and gx_size % 2 == 0
    chips = devices // 2
    highs = camera_count // LOW
    res = interleaved(residual)
    cam_jac = interleaved(jnp.swapaxes(cam_jacobian, 0, 1))
    point_jac = interleaved(jnp.swapaxes(point_jacobian, 0, 1))
    vmem = pl.BlockSpec(memory_space=pltpu.VMEM)
    smem = pl.BlockSpec(memory_space=pltpu.SMEM)
    moved, position, scalars = pl.pallas_call(
        point_kernel,
        out_shape=(
            jax.ShapeDtypeStruct((2, rows, LANES), F32),
            jax.ShapeDtypeStruct((rows, LANES), jnp.int32),
            jax.ShapeDtypeStruct((2, LANES), F32),
        ),
        in_specs=[smem] + [vmem] * 6,
        out_specs=(vmem, vmem, vmem),
        scratch_shapes=[
            pltpu.VMEM((rows * FEATURES, LANES), F32),
            pltpu.VMEM((blocks + 1, FEATURES, LANES), F32),
            pltpu.VMEM((3, blocks + 1, LANES), F32),
        ],
        name="point_part",
    )(
        tile_offset,
        res,
        point_jac,
        obs_camera.reshape(rows, LANES),
        obs_slot.reshape(rows, LANES),
        damping.reshape(blocks, LANES),
        camera_slot.reshape(camera_count // LANES, LANES),
    )
    depth = GROUP * LANES
    dma = pltpu.SemaphoreType.DMA
    reduced, cost, norm = pl.pallas_call(
        functools.partial(
            camera_kernel,
            gx_size,
            gy_size,
            1.0 / (2.0 * n_obs * devices),
            1.0 / (9.0 * camera_count + 3.0 * damping.shape[0] * devices),
        ),
        out_shape=(
            jax.ShapeDtypeStruct((PARAMS, LANES), F32),
            jax.ShapeDtypeStruct((1, 1), F32),
            jax.ShapeDtypeStruct((1, 1), F32),
        ),
        in_specs=[vmem] * 5,
        out_specs=(vmem, vmem, vmem),
        scratch_shapes=[
            pltpu.VMEM((4 * PARAMS * highs, LOW), F32),
            pltpu.VMEM((2, 4 * PARAMS * highs, depth), BF16),
            pltpu.VMEM((2, LOW, depth), BF16),
            pltpu.VMEM((2, 4 * PARAMS, GROUP, LANES), F32),
            pltpu.VMEM((2, chips, 2 * PARAMS, LANES), F32),
            pltpu.VMEM((chips, 2 * PARAMS, LANES), F32),
            pltpu.VMEM((chips, 2 * PARAMS, LANES), F32),
            pltpu.VMEM((chips, 2 * PARAMS, LANES), F32),
            pltpu.VMEM((2, LANES), F32),
            pltpu.VMEM((devices, 2, LANES), F32),
            dma((2,)),
            dma((chips,)),
            dma((chips,)),
            dma((devices,)),
            dma((devices,)),
        ],
        compiler_params=pltpu.CompilerParams(collective_id=0, has_side_effects=True),
        name="camera_part",
    )(cam_jac, res, moved, position, scalars)
    return (reduced, cost.reshape(()), norm.reshape(()))


def solution(mesh):
    return jax.shard_map(
        functools.partial(on_device, mesh.shape["gx"], mesh.shape["gy"]),
        mesh=mesh,
        in_specs=(
            P(None, AXES),
            P(None, None, AXES),
            P(None, None, AXES),
            P(AXES),
            P(AXES),
            P(AXES),
            P(AXES),
            P(),
        ),
        out_specs=(P(None, AXES), P(), P()),
        check_vma=False,
    )
```

```python
import functools

import jax
import jax.numpy as jnp
from jax import lax
from jax.experimental import pallas as pl
from jax.experimental.pallas import tpu as pltpu
from jax.sharding import PartitionSpec as P

AXES = ("gx", "gy")
MESH = pl.DeviceIdType.MESH
F32 = jnp.float32
BF16 = jnp.bfloat16
LANES = 128
GROUP = 8
LOW_BITS = 8
LOW = 1 << LOW_BITS
PARAMS = 9
FEATURES = 16


def nt_dot(left, right):
    return lax.dot_general(left, right, (((1,), (1,)), ((), ())), preferred_element_type=F32)


def split_pieces(value, pieces):
    out = []
    rest = value
    for _ in range(pieces - 1):
        head = rest.astype(BF16)
        out.append(head)
        rest = rest - head.astype(F32)
    out.append(rest.astype(BF16))
    return out


def lane_take(row, index):
    table = jnp.broadcast_to(row, index.shape)
    return jnp.take_along_axis(table, index, axis=1)


def block_solve(entries, rhs):
    comp_aa, comp_ab, comp_ac, comp_bb, comp_bc, comp_cc = entries
    cof_aa = comp_bb * comp_cc - comp_bc * comp_bc
    cof_ab = comp_ac * comp_bc - comp_ab * comp_cc
    cof_ac = comp_ab * comp_bc - comp_ac * comp_bb
    cof_bb = comp_aa * comp_cc - comp_ac * comp_ac
    cof_bc = comp_ab * comp_ac - comp_aa * comp_bc
    cof_cc = comp_aa * comp_bb - comp_ab * comp_ab
    determ = comp_aa * cof_aa + comp_ab * cof_ab + comp_ac * cof_ac
    first = (cof_aa * rhs[0] + cof_ab * rhs[1] + cof_ac * rhs[2]) / determ
    second = (cof_ab * rhs[0] + cof_bb * rhs[1] + cof_bc * rhs[2]) / determ
    third = (cof_ac * rhs[0] + cof_bc * rhs[1] + cof_cc * rhs[2]) / determ
    return first, second, third


def point_kernel(
    toff_ref, res_hbm, pj_hbm, cam_ref, slot_ref, damp_ref, cslot_ref,
    w_ref, pos_ref, scal_ref, feat, sums, steps, res_ref, pj_ref, in_sems,
):
    copies = [
        pltpu.make_async_copy(res_hbm, res_ref, in_sems.at[0]),
        pltpu.make_async_copy(pj_hbm, pj_ref, in_sems.at[1]),
    ]
    for copy in copies:
        copy.start()
    rows = cam_ref.shape[0]
    tiles = toff_ref.shape[0]
    tile_rows = rows // tiles
    blocks = damp_ref.shape[0]
    table_rows = cslot_ref.shape[0]
    groups = rows // GROUP
    per_group = max(1, GROUP // tile_rows)

    sums[...] = jnp.zeros_like(sums)
    feat[...] = jnp.zeros_like(feat)

    def pair(ref, group, lead=()):
        return [
            ref[(*lead, pl.ds(group * (2 * GROUP) + part, GROUP, stride=2), slice(None))]
            for part in range(2)
        ]

    def position_step(group, carry):
        at = pl.ds(pl.multiple_of(group * GROUP, GROUP), GROUP)
        camera = cam_ref[at, :]
        high = camera >> 7
        low = camera & (LANES - 1)
        position = jnp.zeros_like(camera)
        for t in range(table_rows):
            position = jnp.where(high == t, lane_take(cslot_ref[t : t + 1, :], low), position)
        pos_ref[at, :] = position
        return carry

    lax.fori_loop(0, groups, position_step, 0, unroll=4)
    for copy in copies:
        copy.wait()

    def group_step(group, cost):
        res = pair(res_ref, group)
        jac = [pair(pj_ref, group, (k,)) for k in range(3)]
        values = [jac[k][0] * res[0] + jac[k][1] * res[1] for k in range(3)]
        for k, l in ((0, 0), (0, 1), (0, 2), (1, 1), (1, 2), (2, 2)):
            values.append(jac[k][0] * jac[l][0] + jac[k][1] * jac[l][1])
        for f, value in enumerate(values):
            feat[pl.ds(group * (GROUP * FEATURES) + f, GROUP, stride=FEATURES), :] = value
        return cost + (res[0] * res[0] + res[1] * res[1])

    cost = lax.fori_loop(0, groups, group_step, jnp.zeros((GROUP, LANES), F32), unroll=2)

    points = lax.broadcasted_iota(jnp.int32, (LANES, LANES), 0)
    lane = lax.broadcasted_iota(jnp.int32, (FEATURES, LANES), 1)
    batch = 4 if tiles % 4 == 0 else 1

    def tile_batch(step, carry):
        totals = []
        for b in range(batch):
            tile = step * batch + b
            left, right = [], []
            for r in range(tile_rows):
                row = tile * tile_rows + r
                start = pl.multiple_of(row * FEATURES, FEATURES)
                pieces = split_pieces(feat[pl.ds(start, FEATURES), :], 3)
                left.append(jnp.concatenate(pieces, axis=0))
                slot = slot_ref[pl.ds(row, 1), :]
                right.append(jnp.where(points == slot, 1.0, 0.0).astype(BF16))
            out = nt_dot(jnp.concatenate(left, axis=1), jnp.concatenate(right, axis=1))
            totals.append(out[:FEATURES] + out[FEATURES : 2 * FEATURES] + out[2 * FEATURES :])
        for b in range(batch):
            offset = toff_ref[step * batch + b]
            block = offset >> 7
            shift = offset & (LANES - 1)
            rolled = pltpu.roll(totals[b], shift, 1)
            sums[block] += jnp.where(lane >= shift, rolled, 0.0)
            sums[block + 1] += jnp.where(lane < shift, rolled, 0.0)
        return carry

    lax.fori_loop(0, tiles // batch, tile_batch, 0)

    damp = damp_ref[...]
    columns = [sums[pl.ds(0, blocks), f, :] for f in range(9)]
    grad = columns[:3]
    entries = [
        col + damp if i in (0, 3, 5) else col for i, col in enumerate(columns[3:])
    ]
    step_point = block_solve(entries, grad)
    for k in range(3):
        steps[k, pl.ds(0, blocks), :] = step_point[k]
        steps[k, pl.ds(blocks, 1), :] = jnp.zeros((1, LANES), F32)
    square = grad[0] * grad[0] + grad[1] * grad[1] + grad[2] * grad[2]
    scal_ref[0:1, :] = jnp.sum(cost, axis=0, keepdims=True)
    scal_ref[1:2, :] = jnp.sum(square, axis=0, keepdims=True)

    sub = lax.broadcasted_iota(jnp.int32, (GROUP, LANES), 0)

    def take_step(group, carry):
        at = pl.ds(pl.multiple_of(group * GROUP, GROUP), GROUP)
        first = (group * GROUP) // tile_rows
        offsets = [toff_ref[first + t] for t in range(per_group)]
        shift = jnp.zeros((GROUP, LANES), jnp.int32) + (offsets[0] & (LANES - 1))
        for t in range(1, per_group):
            shift = jnp.where(sub >= t * tile_rows, offsets[t] & (LANES - 1), shift)
        index = slot_ref[at, :] + shift
        low = index & (LANES - 1)
        inside = index < LANES
        res = pair(res_ref, group)
        moved = [-res[0], -res[1]]
        for k in range(3):
            here = jnp.broadcast_to(steps[k, pl.ds(offsets[0] >> 7, 1), :], (GROUP, LANES))
            after = jnp.broadcast_to(steps[k, pl.ds((offsets[0] >> 7) + 1, 1), :], (GROUP, LANES))
            for t in range(1, per_group):
                later = sub >= t * tile_rows
                here = jnp.where(later, steps[k, pl.ds(offsets[t] >> 7, 1), :], here)
                after = jnp.where(later, steps[k, pl.ds((offsets[t] >> 7) + 1, 1), :], after)
            taken = jnp.where(
                inside,
                jnp.take_along_axis(here, low, axis=1),
                jnp.take_along_axis(after, low, axis=1),
            )
            jac = pair(pj_ref, group, (k,))
            moved = [moved[a] + jac[a] * taken for a in range(2)]
        w_ref[0, at, :] = moved[0]
        w_ref[1, at, :] = moved[1]
        return carry

    lax.fori_loop(0, groups, take_step, 0, unroll=2)


def camera_kernel(
    gx_size, gy_size, cost_scale, norm_scale,
    cj_hbm, res_ref, w_ref, pos_ref, scal_ref,
    red_ref, cost_ref, norm_ref,
    cj_ref, acc, left, right, rowbuf, part, pair_in, chip_sum, recv, tot_send, tot_recv,
    in_sems, pair_sems, chip_send, chip_recv, tot_ssem, tot_rsem,
):
    devices = gx_size * gy_size
    chips = devices // 2
    gx = lax.axis_index("gx")
    gy = lax.axis_index("gy")
    me = gx * gy_size + gy
    core = lax.rem(gx, 2)
    chip = (gx // 2) * gy_size + gy
    rows = pos_ref.shape[0]
    steps = rows // (2 * GROUP)
    highs = devices * LANES // LOW

    def cj_copy(step):
        at = pl.ds(pl.multiple_of(step * (4 * GROUP), 4 * GROUP), 4 * GROUP)
        return pltpu.make_async_copy(cj_hbm.at[:, at, :], cj_ref.at[:, at, :], in_sems.at[step])

    def cj_start(step, carry):
        cj_copy(step).start()
        return carry

    lax.fori_loop(0, steps, cj_start, 0)

    barrier = pltpu.get_barrier_semaphore()

    def greet(i, carry):
        peer = lax.rem(me + i, devices)
        pl.semaphore_signal(
            barrier, inc=1, device_id=(peer // gy_size, lax.rem(peer, gy_size)), device_id_type=MESH
        )
        return carry

    lax.fori_loop(1, devices, greet, 0)

    lows = lax.broadcasted_iota(jnp.int32, (LOW, LANES), 0)
    tops = lax.broadcasted_iota(jnp.int32, (highs, LANES), 0)
    acc[...] = jnp.zeros_like(acc)

    def add_group(which, group, buf):
        at = pl.ds(pl.multiple_of(group * GROUP, GROUP), GROUP)
        even = pl.ds(group * (2 * GROUP), GROUP, stride=2)
        odd = pl.ds(group * (2 * GROUP) + 1, GROUP, stride=2)
        if which == 0:
            factor0, factor1 = res_ref[even, :], res_ref[odd, :]
        else:
            factor0, factor1 = w_ref[0, at, :], w_ref[1, at, :]
        for m in range(PARAMS):
            value = cj_ref[m, even, :] * factor0 + cj_ref[m, odd, :] * factor1
            head = value.astype(BF16).astype(F32)
            rowbuf[buf, m] = head
            rowbuf[buf, PARAMS + m] = value - head
        for r in range(GROUP):
            position = pos_ref[pl.ds(group * GROUP + r, 1), :]
            cols = slice(r * LANES, (r + 1) * LANES)
            if which == 0:
                onehot = jnp.where(lows == (position & (LOW - 1)), 1.0, 0.0).astype(BF16)
                right[group, :, cols] = onehot
            top = jnp.where(tops == (position >> LOW_BITS), 1.0, 0.0).astype(BF16)
            for j in range(2 * PARAMS):
                row = jnp.broadcast_to(rowbuf[buf, j, r : r + 1, :], (highs, LANES)).astype(BF16)
                left[buf, j * highs : (j + 1) * highs, cols] = row * top
        acc[which] += nt_dot(left[buf], right[group])

    def grad_groups(step, carry):
        cj_copy(step).wait()
        for buf in range(2):
            add_group(0, step * 2 + buf, buf)
        return carry

    def red_groups(step, carry):
        for buf in range(2):
            add_group(1, step * 2 + buf, buf)
        return carry

    def pack(which):
        for dest in range(devices):
            dgx, dgy = dest // gy_size, dest % gy_size
            half = slice((dest % 2) * LANES, (dest % 2 + 1) * LANES)
            for m in range(PARAMS):
                head = m * highs + dest // 2
                rest = (PARAMS + m) * highs + dest // 2
                part[which, dgx % 2, (dgx // 2) * gy_size + dgy, :, m * LANES : (m + 1) * LANES] = (
                    acc[which, head : head + 1, half] + acc[which, rest : rest + 1, half]
                )

    def swap(which):
        return pltpu.make_async_remote_copy(
            src_ref=part.at[which, 1 - core],
            dst_ref=pair_in.at[which],
            send_sem=pair_sems.at[which, 0],
            recv_sem=pair_sems.at[which, 1],
            device_id=(gx + 1 - 2 * core, gy),
            device_id_type=MESH,
        )

    def chip_copy(which, i):
        peer = lax.rem(chip + i, chips)
        return pltpu.make_async_remote_copy(
            src_ref=chip_sum.at[which, peer],
            dst_ref=recv.at[which, i],
            send_sem=chip_send.at[which, i],
            recv_sem=chip_recv.at[which, i],
            device_id=((peer // gy_size) * 2 + core, lax.rem(peer, gy_size)),
            device_id_type=MESH,
        )

    def spread(which):
        swap(which).wait()
        chip_sum[which] = part[which, core] + pair_in[which]

        def chip_start(i, carry):
            chip_copy(which, i).start()
            return carry

        lax.fori_loop(1, chips, chip_start, 0)

    def gather(which):
        def chip_wait(i, total):
            chip_copy(which, i).wait()
            return total + recv[which, i]

        return lax.fori_loop(1, chips, chip_wait, chip_sum[which, chip])

    def tot_copy(i):
        peer = lax.rem(me + i, devices)
        return pltpu.make_async_remote_copy(
            src_ref=tot_send,
            dst_ref=tot_recv.at[me],
            send_sem=tot_ssem.at[i],
            recv_sem=tot_rsem.at[i],
            device_id=(peer // gy_size, lax.rem(peer, gy_size)),
            device_id_type=MESH,
        )

    def tot_start(i, carry):
        tot_copy(i).start()
        return carry

    def tot_wait(i, carry):
        tot_copy(i).wait()
        return carry

    early = steps // 4
    lax.fori_loop(0, steps, grad_groups, 0)
    pack(0)
    pl.semaphore_wait(barrier, devices - 1)
    swap(0).start()
    lax.fori_loop(0, early, red_groups, 0)
    spread(0)
    lax.fori_loop(early, steps, red_groups, 0)
    pack(1)
    swap(1).start()

    grad = gather(0)
    square = jnp.zeros((1, LANES), F32)
    for m in range(PARAMS):
        column = grad[:, m * LANES : (m + 1) * LANES]
        square = square + column * column
    tot_send[0:1, :] = scal_ref[0:1, :]
    tot_send[1:2, :] = scal_ref[1:2, :] + square
    tot_recv[me] = tot_send[...]
    lax.fori_loop(1, devices, tot_start, 0)

    spread(1)
    reduced = gather(1)
    for m in range(PARAMS):
        red_ref[m : m + 1, :] = reduced[:, m * LANES : (m + 1) * LANES]

    lax.fori_loop(1, devices, tot_wait, 0)
    sums = tot_recv[0]
    for d in range(1, devices):
        sums = sums + tot_recv[d]
    sums = jnp.sum(sums, axis=1, keepdims=True)
    cost_ref[...] = sums[0:1] * cost_scale
    norm_ref[...] = jnp.sqrt(sums[1:2] * norm_scale + 1e-06)


def interleaved(array):
    lead = array.shape[:-2]
    n_obs = array.shape[-1]
    blocks = array.reshape(*lead, 2, n_obs // LANES, LANES)
    return jnp.swapaxes(blocks, -3, -2).reshape(*lead, 2 * n_obs // LANES, LANES)


def on_device(
    gx_size, gy_size,
    residual, cam_jacobian, point_jacobian, obs_camera, obs_slot, tile_offset, damping, camera_slot
):
    devices = gx_size * gy_size
    n_obs = residual.shape[1]
    rows = n_obs // LANES
    blocks = damping.shape[0] // LANES
    camera_count = camera_slot.shape[0]
    assert camera_count == devices * LANES and gx_size % 2 == 0
    chips = devices // 2
    highs = camera_count // LOW
    res = interleaved(residual)
    cam_jac = interleaved(jnp.swapaxes(cam_jacobian, 0, 1))
    point_jac = interleaved(jnp.swapaxes(point_jacobian, 0, 1))
    vmem = pl.BlockSpec(memory_space=pltpu.VMEM)
    hbm = pl.BlockSpec(memory_space=pl.ANY)
    smem = pl.BlockSpec(memory_space=pltpu.SMEM)
    moved, position, scalars = pl.pallas_call(
        point_kernel,
        out_shape=(
            jax.ShapeDtypeStruct((2, rows, LANES), F32),
            jax.ShapeDtypeStruct((rows, LANES), jnp.int32),
            jax.ShapeDtypeStruct((2, LANES), F32),
        ),
        in_specs=[smem, hbm, hbm] + [vmem] * 4,
        out_specs=(vmem, vmem, vmem),
        scratch_shapes=[
            pltpu.VMEM((rows * FEATURES, LANES), F32),
            pltpu.VMEM((blocks + 1, FEATURES, LANES), F32),
            pltpu.VMEM((3, blocks + 1, LANES), F32),
            pltpu.VMEM(res.shape, F32),
            pltpu.VMEM(point_jac.shape, F32),
            pltpu.SemaphoreType.DMA((2,)),
        ],
        name="point_part",
    )(
        tile_offset,
        res,
        point_jac,
        obs_camera.reshape(rows, LANES),
        obs_slot.reshape(rows, LANES),
        damping.reshape(blocks, LANES),
        camera_slot.reshape(camera_count // LANES, LANES),
    )
    depth = GROUP * LANES
    dma = pltpu.SemaphoreType.DMA
    reduced, cost, norm = pl.pallas_call(
        functools.partial(
            camera_kernel,
            gx_size,
            gy_size,
            1.0 / (2.0 * n_obs * devices),
            1.0 / (9.0 * camera_count + 3.0 * damping.shape[0] * devices),
        ),
        out_shape=(
            jax.ShapeDtypeStruct((PARAMS, LANES), F32),
            jax.ShapeDtypeStruct((1, 1), F32),
            jax.ShapeDtypeStruct((1, 1), F32),
        ),
        in_specs=[hbm] + [vmem] * 4,
        out_specs=(vmem, vmem, vmem),
        scratch_shapes=[
            pltpu.VMEM(cam_jac.shape, F32),
            pltpu.VMEM((2, 2 * PARAMS * highs, LOW), F32),
            pltpu.VMEM((2, 2 * PARAMS * highs, depth), BF16),
            pltpu.VMEM((rows // GROUP, LOW, depth), BF16),
            pltpu.VMEM((2, 2 * PARAMS, GROUP, LANES), F32),
            pltpu.VMEM((2, 2, chips, 1, PARAMS * LANES), F32),
            pltpu.VMEM((2, chips, 1, PARAMS * LANES), F32),
            pltpu.VMEM((2, chips, 1, PARAMS * LANES), F32),
            pltpu.VMEM((2, chips, 1, PARAMS * LANES), F32),
            pltpu.VMEM((2, LANES), F32),
            pltpu.VMEM((devices, 2, LANES), F32),
            dma((rows // (2 * GROUP),)),
            dma((2, 2)),
            dma((2, chips)),
            dma((2, chips)),
            dma((devices,)),
            dma((devices,)),
        ],
        compiler_params=pltpu.CompilerParams(collective_id=0, has_side_effects=True),
        name="camera_part",
    )(cam_jac, res, moved, position, scalars)
    return (reduced, cost.reshape(()), norm.reshape(()))


def solution(mesh):
    return jax.shard_map(
        functools.partial(on_device, mesh.shape["gx"], mesh.shape["gy"]),
        mesh=mesh,
        in_specs=(
            P(None, AXES),
            P(None, None, AXES),
            P(None, None, AXES),
            P(AXES),
            P(AXES),
            P(AXES),
            P(AXES),
            P(),
        ),
        out_specs=(P(None, AXES), P(), P()),
        check_vma=False,
    )
```

```python
import functools

import jax
import jax.numpy as jnp
from jax import lax
from jax.experimental import pallas as pl
from jax.experimental.pallas import tpu as pltpu
from jax.sharding import PartitionSpec as P

AXES = ("gx", "gy")
MESH = pl.DeviceIdType.MESH
F32 = jnp.float32
BF16 = jnp.bfloat16
LANES = 128
GROUP = 8
SLOTS = 2
LOW_BITS = 8
LOW = 1 << LOW_BITS
PARAMS = 9
FEATURES = 16


def nt_dot(left, right):
    return lax.dot_general(left, right, (((1,), (1,)), ((), ())), preferred_element_type=F32)


def split_pieces(value, pieces):
    out = []
    rest = value
    for _ in range(pieces - 1):
        head = rest.astype(BF16)
        out.append(head)
        rest = rest - head.astype(F32)
    out.append(rest.astype(BF16))
    return out


def lane_take(row, index):
    table = jnp.broadcast_to(row, index.shape)
    return jnp.take_along_axis(table, index, axis=1)


def block_solve(entries, rhs):
    comp_aa, comp_ab, comp_ac, comp_bb, comp_bc, comp_cc = entries
    cof_aa = comp_bb * comp_cc - comp_bc * comp_bc
    cof_ab = comp_ac * comp_bc - comp_ab * comp_cc
    cof_ac = comp_ab * comp_bc - comp_ac * comp_bb
    cof_bb = comp_aa * comp_cc - comp_ac * comp_ac
    cof_bc = comp_ab * comp_ac - comp_aa * comp_bc
    cof_cc = comp_aa * comp_bb - comp_ab * comp_ab
    determ = comp_aa * cof_aa + comp_ab * cof_ab + comp_ac * cof_ac
    first = (cof_aa * rhs[0] + cof_ab * rhs[1] + cof_ac * rhs[2]) / determ
    second = (cof_ab * rhs[0] + cof_bb * rhs[1] + cof_bc * rhs[2]) / determ
    third = (cof_ac * rhs[0] + cof_bc * rhs[1] + cof_cc * rhs[2]) / determ
    return first, second, third


def point_kernel(
    toff_ref, res_hbm, pj_hbm, cam_ref, slot_ref, damp_ref, cslot_ref,
    w_ref, pos_ref, scal_ref, feat, sums, steps, res_ref, pj_ref, in_sems,
):
    copies = [
        pltpu.make_async_copy(res_hbm, res_ref, in_sems.at[0]),
        pltpu.make_async_copy(pj_hbm, pj_ref, in_sems.at[1]),
    ]
    for copy in copies:
        copy.start()
    rows = cam_ref.shape[0]
    tiles = toff_ref.shape[0]
    tile_rows = rows // tiles
    blocks = damp_ref.shape[0]
    table_rows = cslot_ref.shape[0]
    groups = rows // GROUP
    per_group = max(1, GROUP // tile_rows)

    sums[...] = jnp.zeros_like(sums)
    feat[...] = jnp.zeros_like(feat)

    def pair(ref, group, lead=()):
        return [
            ref[(*lead, pl.ds(group * (2 * GROUP) + part, GROUP, stride=2), slice(None))]
            for part in range(2)
        ]

    def position_step(group, carry):
        at = pl.ds(pl.multiple_of(group * GROUP, GROUP), GROUP)
        camera = cam_ref[at, :]
        high = camera >> 7
        low = camera & (LANES - 1)
        position = jnp.zeros_like(camera)
        for t in range(table_rows):
            position = jnp.where(high == t, lane_take(cslot_ref[t : t + 1, :], low), position)
        pos_ref[0, at, :] = (position & (LOW - 1)).astype(F32)
        pos_ref[1, at, :] = (position >> LOW_BITS).astype(F32)
        return carry

    lax.fori_loop(0, groups, position_step, 0, unroll=4)
    for copy in copies:
        copy.wait()

    def group_step(group, cost):
        res = pair(res_ref, group)
        jac = [pair(pj_ref, group, (k,)) for k in range(3)]
        values = [jac[k][0] * res[0] + jac[k][1] * res[1] for k in range(3)]
        for k, l in ((0, 0), (0, 1), (0, 2), (1, 1), (1, 2), (2, 2)):
            values.append(jac[k][0] * jac[l][0] + jac[k][1] * jac[l][1])
        for f, value in enumerate(values):
            feat[pl.ds(group * (GROUP * FEATURES) + f, GROUP, stride=FEATURES), :] = value
        return cost + (res[0] * res[0] + res[1] * res[1])

    cost = lax.fori_loop(0, groups, group_step, jnp.zeros((GROUP, LANES), F32), unroll=2)

    points = lax.broadcasted_iota(jnp.int32, (LANES, LANES), 0)
    lane = lax.broadcasted_iota(jnp.int32, (FEATURES, LANES), 1)
    batch = 4 if tiles % 4 == 0 else 1

    def tile_batch(step, carry):
        totals = []
        for b in range(batch):
            tile = step * batch + b
            left, right = [], []
            for r in range(tile_rows):
                row = tile * tile_rows + r
                start = pl.multiple_of(row * FEATURES, FEATURES)
                pieces = split_pieces(feat[pl.ds(start, FEATURES), :], 3)
                left.append(jnp.concatenate(pieces, axis=0))
                slot = slot_ref[pl.ds(row, 1), :]
                right.append(jnp.where(points == slot, 1.0, 0.0).astype(BF16))
            out = nt_dot(jnp.concatenate(left, axis=1), jnp.concatenate(right, axis=1))
            totals.append(out[:FEATURES] + out[FEATURES : 2 * FEATURES] + out[2 * FEATURES :])
        for b in range(batch):
            offset = toff_ref[step * batch + b]
            block = offset >> 7
            shift = offset & (LANES - 1)
            rolled = pltpu.roll(totals[b], shift, 1)
            sums[block] += jnp.where(lane >= shift, rolled, 0.0)
            sums[block + 1] += jnp.where(lane < shift, rolled, 0.0)
        return carry

    lax.fori_loop(0, tiles // batch, tile_batch, 0)

    damp = damp_ref[...]
    columns = [sums[pl.ds(0, blocks), f, :] for f in range(9)]
    grad = columns[:3]
    entries = [
        col + damp if i in (0, 3, 5) else col for i, col in enumerate(columns[3:])
    ]
    step_point = block_solve(entries, grad)
    for k in range(3):
        steps[k, pl.ds(0, blocks), :] = step_point[k]
        steps[k, pl.ds(blocks, 1), :] = jnp.zeros((1, LANES), F32)
    square = grad[0] * grad[0] + grad[1] * grad[1] + grad[2] * grad[2]
    scal_ref[0:1, :] = jnp.sum(cost, axis=0, keepdims=True)
    scal_ref[1:2, :] = jnp.sum(square, axis=0, keepdims=True)

    sub = lax.broadcasted_iota(jnp.int32, (GROUP, LANES), 0)

    def take_step(group, carry):
        at = pl.ds(pl.multiple_of(group * GROUP, GROUP), GROUP)
        first = (group * GROUP) // tile_rows
        offsets = [toff_ref[first + t] for t in range(per_group)]
        shift = jnp.zeros((GROUP, LANES), jnp.int32) + (offsets[0] & (LANES - 1))
        for t in range(1, per_group):
            shift = jnp.where(sub >= t * tile_rows, offsets[t] & (LANES - 1), shift)
        index = slot_ref[at, :] + shift
        low = index & (LANES - 1)
        inside = index < LANES
        res = pair(res_ref, group)
        moved = [-res[0], -res[1]]
        for k in range(3):
            here = jnp.broadcast_to(steps[k, pl.ds(offsets[0] >> 7, 1), :], (GROUP, LANES))
            after = jnp.broadcast_to(steps[k, pl.ds((offsets[0] >> 7) + 1, 1), :], (GROUP, LANES))
            for t in range(1, per_group):
                later = sub >= t * tile_rows
                here = jnp.where(later, steps[k, pl.ds(offsets[t] >> 7, 1), :], here)
                after = jnp.where(later, steps[k, pl.ds((offsets[t] >> 7) + 1, 1), :], after)
            taken = jnp.where(
                inside,
                jnp.take_along_axis(here, low, axis=1),
                jnp.take_along_axis(after, low, axis=1),
            )
            jac = pair(pj_ref, group, (k,))
            moved = [moved[a] + jac[a] * taken for a in range(2)]
        w_ref[0, at, :] = moved[0]
        w_ref[1, at, :] = moved[1]
        return carry

    lax.fori_loop(0, groups, take_step, 0, unroll=2)


def camera_kernel(
    gx_size, gy_size, cost_scale, norm_scale,
    cj_hbm, res_ref, w_ref, pos_ref, scal_ref,
    red_ref, cost_ref, norm_ref,
    cj_ref, acc, left, right, rowbuf, part, pair_in, chip_sum, recv, tot_send, tot_recv,
    in_sems, pair_sems, chip_send, chip_recv, tot_ssem, tot_rsem,
):
    devices = gx_size * gy_size
    chips = devices // 2
    gx = lax.axis_index("gx")
    gy = lax.axis_index("gy")
    me = gx * gy_size + gy
    core = lax.rem(gx, 2)
    chip = (gx // 2) * gy_size + gy
    rows = pos_ref.shape[1]
    steps = rows // (2 * GROUP)
    highs = devices * LANES // LOW

    def cj_copy(step):
        at = pl.ds(pl.multiple_of(step * (4 * GROUP), 4 * GROUP), 4 * GROUP)
        return pltpu.make_async_copy(cj_hbm.at[:, at, :], cj_ref.at[:, at, :], in_sems.at[step])

    def cj_start(step, carry):
        cj_copy(step).start()
        return carry

    lax.fori_loop(0, steps, cj_start, 0)

    barrier = pltpu.get_barrier_semaphore()

    def greet(i, carry):
        peer = lax.rem(me + i, devices)
        pl.semaphore_signal(
            barrier, inc=1, device_id=(peer // gy_size, lax.rem(peer, gy_size)), device_id_type=MESH
        )
        return carry

    lax.fori_loop(1, devices, greet, 0)

    lows = lax.broadcasted_iota(jnp.int32, (LOW, LANES), 0).astype(F32).astype(BF16)
    tops = lax.broadcasted_iota(jnp.int32, (highs, LANES), 0).astype(F32).astype(BF16)
    one = jnp.ones((), BF16)
    none = jnp.zeros((), BF16)
    acc[...] = jnp.zeros_like(acc)

    def add_group(which, group, buf):
        at = pl.ds(pl.multiple_of(group * GROUP, GROUP), GROUP)
        even = pl.ds(group * (2 * GROUP), GROUP, stride=2)
        odd = pl.ds(group * (2 * GROUP) + 1, GROUP, stride=2)
        if which == 0:
            factor0, factor1 = res_ref[even, :], res_ref[odd, :]
        else:
            factor0, factor1 = w_ref[0, at, :], w_ref[1, at, :]
        for m in range(PARAMS):
            value = cj_ref[m, even, :] * factor0 + cj_ref[m, odd, :] * factor1
            head = value.astype(BF16).astype(F32)
            rowbuf[buf, m] = head
            rowbuf[buf, PARAMS + m] = value - head
        for r in range(GROUP):
            row_at = pl.ds(group * GROUP + r, 1)
            cols = slice(r * LANES, (r + 1) * LANES)
            if which == 0:
                low = jnp.broadcast_to(pos_ref[0, row_at, :], (LOW, LANES)).astype(BF16)
                right[group, :, cols] = jnp.where(lows == low, one, none)
            high = jnp.broadcast_to(pos_ref[1, row_at, :], (highs, LANES)).astype(BF16)
            top = jnp.where(tops == high, one, none)
            for j in range(2 * PARAMS):
                row = jnp.broadcast_to(rowbuf[buf, j, r : r + 1, :], (highs, LANES)).astype(BF16)
                left[buf, j * highs : (j + 1) * highs, cols] = row * top
        acc[which] += nt_dot(left[buf], right[group])

    def grad_groups(step, carry):
        for buf in range(SLOTS):
            if buf % 2 == 0:
                cj_copy(step * (SLOTS // 2) + buf // 2).wait()
            add_group(0, step * SLOTS + buf, buf)
        return carry

    def red_groups(step, carry):
        for buf in range(SLOTS):
            add_group(1, step * SLOTS + buf, buf)
        return carry

    def pack(which):
        for dest in range(devices):
            dgx, dgy = dest // gy_size, dest % gy_size
            half = slice((dest % 2) * LANES, (dest % 2 + 1) * LANES)
            for m in range(PARAMS):
                head = m * highs + dest // 2
                rest = (PARAMS + m) * highs + dest // 2
                part[which, dgx % 2, (dgx // 2) * gy_size + dgy, :, m * LANES : (m + 1) * LANES] = (
                    acc[which, head : head + 1, half] + acc[which, rest : rest + 1, half]
                )

    def swap(which):
        return pltpu.make_async_remote_copy(
            src_ref=part.at[which, 1 - core],
            dst_ref=pair_in.at[which],
            send_sem=pair_sems.at[which, 0],
            recv_sem=pair_sems.at[which, 1],
            device_id=(gx + 1 - 2 * core, gy),
            device_id_type=MESH,
        )

    def chip_copy(which, i):
        peer = lax.rem(chip + i, chips)
        return pltpu.make_async_remote_copy(
            src_ref=chip_sum.at[which, peer],
            dst_ref=recv.at[which, i],
            send_sem=chip_send.at[which, i],
            recv_sem=chip_recv.at[which, i],
            device_id=((peer // gy_size) * 2 + core, lax.rem(peer, gy_size)),
            device_id_type=MESH,
        )

    def spread(which):
        swap(which).wait()
        chip_sum[which] = part[which, core] + pair_in[which]

        def chip_start(i, carry):
            chip_copy(which, i).start()
            return carry

        lax.fori_loop(1, chips, chip_start, 0)

    def gather(which):
        def chip_wait(i, total):
            chip_copy(which, i).wait()
            return total + recv[which, i]

        return lax.fori_loop(1, chips, chip_wait, chip_sum[which, chip])

    def tot_copy(i):
        peer = lax.rem(me + i, devices)
        return pltpu.make_async_remote_copy(
            src_ref=tot_send,
            dst_ref=tot_recv.at[me],
            send_sem=tot_ssem.at[i],
            recv_sem=tot_rsem.at[i],
            device_id=(peer // gy_size, lax.rem(peer, gy_size)),
            device_id_type=MESH,
        )

    def tot_start(i, carry):
        tot_copy(i).start()
        return carry

    def tot_wait(i, carry):
        tot_copy(i).wait()
        return carry

    loops = rows // (SLOTS * GROUP)
    early = loops // 4
    lax.fori_loop(0, loops, grad_groups, 0)
    pack(0)
    pl.semaphore_wait(barrier, devices - 1)
    swap(0).start()
    lax.fori_loop(0, early, red_groups, 0)
    spread(0)
    lax.fori_loop(early, loops, red_groups, 0)
    pack(1)
    swap(1).start()

    grad = gather(0)
    square = jnp.zeros((1, LANES), F32)
    for m in range(PARAMS):
        column = grad[:, m * LANES : (m + 1) * LANES]
        square = square + column * column
    tot_send[0:1, :] = scal_ref[0:1, :]
    tot_send[1:2, :] = scal_ref[1:2, :] + square
    tot_recv[me] = tot_send[...]
    lax.fori_loop(1, devices, tot_start, 0)

    spread(1)
    reduced = gather(1)
    for m in range(PARAMS):
        red_ref[m : m + 1, :] = reduced[:, m * LANES : (m + 1) * LANES]

    lax.fori_loop(1, devices, tot_wait, 0)
    sums = tot_recv[0]
    for d in range(1, devices):
        sums = sums + tot_recv[d]
    sums = jnp.sum(sums, axis=1, keepdims=True)
    cost_ref[...] = sums[0:1] * cost_scale
    norm_ref[...] = jnp.sqrt(sums[1:2] * norm_scale + 1e-06)


def interleaved(array):
    lead = array.shape[:-2]
    n_obs = array.shape[-1]
    blocks = array.reshape(*lead, 2, n_obs // LANES, LANES)
    return jnp.swapaxes(blocks, -3, -2).reshape(*lead, 2 * n_obs // LANES, LANES)


def on_device(
    gx_size, gy_size,
    residual, cam_jacobian, point_jacobian, obs_camera, obs_slot, tile_offset, damping, camera_slot
):
    devices = gx_size * gy_size
    n_obs = residual.shape[1]
    rows = n_obs // LANES
    blocks = damping.shape[0] // LANES
    camera_count = camera_slot.shape[0]
    assert camera_count == devices * LANES and gx_size % 2 == 0
    chips = devices // 2
    highs = camera_count // LOW
    res = interleaved(residual)
    cam_jac = interleaved(jnp.swapaxes(cam_jacobian, 0, 1))
    point_jac = interleaved(jnp.swapaxes(point_jacobian, 0, 1))
    vmem = pl.BlockSpec(memory_space=pltpu.VMEM)
    hbm = pl.BlockSpec(memory_space=pl.ANY)
    smem = pl.BlockSpec(memory_space=pltpu.SMEM)
    moved, position, scalars = pl.pallas_call(
        point_kernel,
        out_shape=(
            jax.ShapeDtypeStruct((2, rows, LANES), F32),
            jax.ShapeDtypeStruct((2, rows, LANES), F32),
            jax.ShapeDtypeStruct((2, LANES), F32),
        ),
        in_specs=[smem, hbm, hbm] + [vmem] * 4,
        out_specs=(vmem, vmem, vmem),
        scratch_shapes=[
            pltpu.VMEM((rows * FEATURES, LANES), F32),
            pltpu.VMEM((blocks + 1, FEATURES, LANES), F32),
            pltpu.VMEM((3, blocks + 1, LANES), F32),
            pltpu.VMEM(res.shape, F32),
            pltpu.VMEM(point_jac.shape, F32),
            pltpu.SemaphoreType.DMA((2,)),
        ],
        name="point_part",
    )(
        tile_offset,
        res,
        point_jac,
        obs_camera.reshape(rows, LANES),
        obs_slot.reshape(rows, LANES),
        damping.reshape(blocks, LANES),
        camera_slot.reshape(camera_count // LANES, LANES),
    )
    depth = GROUP * LANES
    dma = pltpu.SemaphoreType.DMA
    reduced, cost, norm = pl.pallas_call(
        functools.partial(
            camera_kernel,
            gx_size,
            gy_size,
            1.0 / (2.0 * n_obs * devices),
            1.0 / (9.0 * camera_count + 3.0 * damping.shape[0] * devices),
        ),
        out_shape=(
            jax.ShapeDtypeStruct((PARAMS, LANES), F32),
            jax.ShapeDtypeStruct((1, 1), F32),
            jax.ShapeDtypeStruct((1, 1), F32),
        ),
        in_specs=[hbm] + [vmem] * 4,
        out_specs=(vmem, vmem, vmem),
        scratch_shapes=[
            pltpu.VMEM(cam_jac.shape, F32),
            pltpu.VMEM((2, 2 * PARAMS * highs, LOW), F32),
            pltpu.VMEM((SLOTS, 2 * PARAMS * highs, depth), BF16),
            pltpu.VMEM((rows // GROUP, LOW, depth), BF16),
            pltpu.VMEM((SLOTS, 2 * PARAMS, GROUP, LANES), F32),
            pltpu.VMEM((2, 2, chips, 1, PARAMS * LANES), F32),
            pltpu.VMEM((2, chips, 1, PARAMS * LANES), F32),
            pltpu.VMEM((2, chips, 1, PARAMS * LANES), F32),
            pltpu.VMEM((2, chips, 1, PARAMS * LANES), F32),
            pltpu.VMEM((2, LANES), F32),
            pltpu.VMEM((devices, 2, LANES), F32),
            dma((rows // (2 * GROUP),)),
            dma((2, 2)),
            dma((2, chips)),
            dma((2, chips)),
            dma((devices,)),
            dma((devices,)),
        ],
        compiler_params=pltpu.CompilerParams(collective_id=0, has_side_effects=True),
        name="camera_part",
    )(cam_jac, res, moved, position, scalars)
    return (reduced, cost.reshape(()), norm.reshape(()))


def solution(mesh):
    return jax.shard_map(
        functools.partial(on_device, mesh.shape["gx"], mesh.shape["gy"]),
        mesh=mesh,
        in_specs=(
            P(None, AXES),
            P(None, None, AXES),
            P(None, None, AXES),
            P(AXES),
            P(AXES),
            P(AXES),
            P(AXES),
            P(),
        ),
        out_specs=(P(None, AXES), P(), P()),
        check_vma=False,
    )
```
